32 devices in a mesh: lon: 16 (over z, y, core), lat: 2 (over x).
Axes of the slice: x: 2, y: 2, z: 4, core: 2. Of those that a mesh axis runs over, the one named last changes fastest.
Arguments:
- fine_members: bfloat16 [32, 64, 256], P(None, 'lon', 'lat'), may hold values from -6 to 6
- coarse_members: bfloat16 [128, 32, 256], P(None, 'lon', 'lat'), may hold values from -6 to 6
- increments: bfloat16 [32, 64, 256], P(None, 'lon', 'lat'), may hold values from -0.59765625 to 0.59765625
- level_weights: float32 [2], replicated, may hold values from 0.5 to 2
Outputs:
- applied: float32 [32, 64, 256], P(None, 'lon', 'lat')
The draws below stay inside these ranges and needn't reach their ends.
All inputs are finite; a program needn't handle non-finite values.
Results may differ from the reference program's by a relative error of at most 0.0055.
Values may be sent and summed in bfloat16 or wider, within the bound.
A program may use at most 64 MiB of HBM per device.

```python
import math
import jax
import jax.numpy as jnp
from jax import lax

CLON = 4
CLAT = 128
KF = 32
KC = 128
NV = 32
NLON = 64
NLAT = 256
N_LON = 16
N_LAT = 2


def steps_of(stream_key, shape, pieces, smallest, high):
    gain, own = 1.0, jax.random.fold_in(stream_key, 6)
    for dim, parts in pieces:
        draws = jnp.exp(jax.random.uniform(jax.random.fold_in(own, dim), (parts,), jnp.float32, smallest / len(pieces), high / len(pieces)))
        gain = gain * jnp.repeat(draws, shape[dim] // parts).reshape([-1 if axis == dim else 1 for axis in range(len(shape))])
    return gain


def bell_draw(own_key, shape, deviation, limit, split=(), kind=jnp.bfloat16):
    array = deviation * jax.random.normal(own_key, shape, jnp.float32)
    if split:
        array = array * steps_of(own_key, shape, split, -0.22, 0.18)
    return jnp.clip(array, -limit, limit).astype(kind)


def setup_inputs(seed: int = 0) -> dict:
    keys = jax.random.split(jax.random.key(seed), 5)
    return {
        "fine_members": bell_draw(keys[0], (KF, NLON, NLAT), 1.0, 6.0, ((1, 16), (2, 2))),
        "coarse_members": bell_draw(keys[1], (KC, NLON // 2, NLAT), 1.0, 6.0, ((1, 16), (2, 2))),
        "increments": bell_draw(keys[2], (NV, NLON, NLAT), 0.1, 0.59765625, ((1, 16), (2, 2))),
        "level_weights": jnp.clip(jnp.exp(jax.random.uniform(keys[3], (2,), jnp.float32, math.log(0.5), math.log(2.0))), 0.5, 2.0),
    }


def refine(coarse):
    left_cols = coarse[:, :-1, :]
    right_cols = coarse[:, 1:, :]
    middle = 0.5 * (left_cols + right_cols)
    stacked = jnp.stack((left_cols, middle), axis=2)
    return stacked.reshape(left_cols.shape[0], 2 * left_cols.shape[1], left_cols.shape[2])


def anomalies(members):
    return (members - jnp.mean(members, axis=0, keepdims=True)).astype(jnp.bfloat16)


def profile(distance, extent):
    ratio = distance.astype(jnp.float32) / extent
    return jnp.where(jnp.abs(distance) <= extent, 1.0 - 0.75 * ratio * ratio, 0.0).astype(jnp.float32)


def reference(fine_members, coarse_members, increments, level_weights):
    lon_reach = CLON - 1
    lat_reach = CLAT // 8
    ext_width = CLAT + 2 * lat_reach
    extended = jnp.concatenate((coarse_members, coarse_members[:, :1, :]), axis=1).astype(jnp.float32)
    refined = refine(extended)
    fine_anom = anomalies(fine_members.astype(jnp.float32))
    coarse_anom = anomalies(refined)
    paired_anom = anomalies(refined[:KF])
    stacked = jnp.concatenate((fine_anom, coarse_anom, paired_anom, increments), axis=0)
    padded = jnp.pad(stacked, ((0, 0), (0, 0), (lat_reach, lat_reach)))
    padded = jnp.concatenate((padded[:, -CLON:], padded, padded[:, :CLON]), axis=1)
    lon_profile = profile(jnp.arange(3 * CLON, dtype=jnp.int32)[None, :] - CLON - jnp.arange(CLON, dtype=jnp.int32)[:, None], lon_reach)
    lat_profile = profile(jnp.arange(ext_width, dtype=jnp.int32)[None, :] - lat_reach - jnp.arange(CLAT, dtype=jnp.int32)[:, None], lat_reach)
    taper = (lon_profile[:, None, :, None] * lat_profile[None, :, None, :]).reshape(CLON * CLAT, 3 * CLON * ext_width)
    weight_fine = level_weights[0] / (KF - 1)
    weight_coarse = level_weights[1] / (KC - 1)
    weight_paired = level_weights[1] / (KF - 1)
    member_rows = 2 * KF + KC
    total_rows = member_rows + NV

    def one_tile(index):
        lon_tile = index // N_LAT
        lat_tile = index % N_LAT
        zero_start = jnp.int32(0)
        hood = lax.dynamic_slice(padded, (zero_start, (lon_tile * CLON).astype(jnp.int32), (lat_tile * CLAT).astype(jnp.int32)), (total_rows, 3 * CLON, ext_width))
        own = lax.dynamic_slice(stacked, (zero_start, (lon_tile * CLON).astype(jnp.int32), (lat_tile * CLAT).astype(jnp.int32)), (member_rows, CLON, CLAT))
        hood = hood.reshape(total_rows, 3 * CLON * ext_width)
        own = own.reshape(member_rows, CLON * CLAT)
        first = jnp.dot(own[:KF].T, hood[:KF], preferred_element_type=jnp.float32)
        second = jnp.dot(own[KF:KF + KC].T, hood[KF:KF + KC], preferred_element_type=jnp.float32)
        third = jnp.dot(own[KF + KC:].T, hood[KF + KC:member_rows], preferred_element_type=jnp.float32)
        gram_tile = weight_fine * first + weight_coarse * second - weight_paired * third
        tapered = (taper * gram_tile).astype(jnp.bfloat16)
        return jnp.dot(hood[member_rows:], tapered.T, preferred_element_type=jnp.float32)

    results = lax.map(one_tile, jnp.arange(N_LON * N_LAT, dtype=jnp.int32))
    results = results.reshape(N_LON, N_LAT, NV, CLON, CLAT)
    return jnp.transpose(results, (2, 0, 3, 1, 4)).reshape(NV, N_LON * CLON, N_LAT * CLAT)
```

```python
import functools

import jax
import jax.numpy as jnp
from jax import lax
from jax.experimental import pallas as pl
from jax.experimental.pallas import tpu as pltpu
from jax.sharding import PartitionSpec as P

MESH = pl.DeviceIdType.MESH
F32, BF16 = jnp.float32, jnp.bfloat16


def profile(distance, extent):
    ratio = distance.astype(F32) / extent
    return jnp.where(jnp.abs(distance) <= extent, 1.0 - 0.75 * ratio * ratio, 0.0)


def iota(shape, dim):
    return lax.broadcasted_iota(jnp.int32, shape, dim)


def kernel(
    sizes, w_ref, fine_ref, coarse_ref, inc_ref, out_ref,
    fine_in, coarse_in, inc_in, wide, own, west, east, rim_out, rim_in,
    near, near_inc, own_t, near_rim, rim_inc, taper, rim_taper, refine_rim, acc,
    in_sem, send_sem, recv_sem, rim_send_sem, rim_recv_sem,
):
    n_lon, n_lat, kf, kc, nv, lons, lats = sizes
    halves, reach, lon_reach = lons // 2, lats // 8, lons - 1
    members = 2 * kf + kc
    col = kf + nv
    groups = kc // kf
    body = lon_reach * col + halves * kc
    coarse_at = lon_reach * col
    lon, lat = lax.axis_index("lon"), lax.axis_index("lat")
    sides = (lax.rem(lon + n_lon - 1, n_lon), lon, lax.rem(lon + 1, n_lon))
    has = (lat > 0, lat < n_lat - 1)

    barrier = pltpu.get_barrier_semaphore()

    def greet(to_lon, to_lat):
        pl.semaphore_signal(barrier, inc=1, device_id=(to_lon, to_lat), device_id_type=MESH)

    greet(sides[0], lat)
    greet(sides[2], lat)
    for s in range(2):
        @pl.when(has[s])
        def _():
            for t in range(3):
                greet(sides[t], lat + 2 * s - 1)

    loads = [
        pltpu.make_async_copy(src, dst, in_sem.at[n])
        for n, (src, dst) in enumerate(
            ((fine_ref, fine_in), (coarse_ref, coarse_in), (inc_ref, inc_in))
        )
    ]
    for load in loads:
        load.start()

    f_at, c_at, i_at = 0, kf * lons, kf * lons + kc * halves

    def column_at(a):
        return a * col if a < lon_reach else body

    loads[0].wait()
    wide[f_at:f_at + kf * lons] = fine_in[...].astype(F32)
    loads[1].wait()
    wide[c_at:c_at + kc * halves] = coarse_in[...].astype(F32)
    loads[2].wait()
    wide[i_at:i_at + nv * lons] = inc_in[...].astype(F32)

    fine_own, inc_own, coarse_own = [], [], []
    for a in range(lons):
        values = wide[pl.ds(f_at + a, kf, stride=lons), :]
        anom = (values - jnp.mean(values, axis=0, keepdims=True)).astype(BF16)
        vectors = wide[pl.ds(i_at + a, nv, stride=lons), :].astype(BF16)
        at = column_at(a)
        own[at:at + kf] = anom
        own[at + kf:at + col] = vectors
        fine_own.append(anom)
        inc_own.append(vectors)
    for c in range(halves):
        values = wide[pl.ds(c_at + c, kc, stride=halves), :]
        own[coarse_at + c * kc:coarse_at + (c + 1) * kc] = values.astype(BF16)
        coarse_own.append(values)

    lane = iota((kf, lats), 1)
    packs = (
        [v.astype(F32) for v in fine_own] + [v.astype(F32) for v in inc_own],
        [coarse_own[c][g * kf:(g + 1) * kf] for g in range(groups) for c in range(halves)],
    )
    for part in range(2):
        low = high = jnp.zeros((kf, lats), F32)
        for q, values in enumerate(packs[part]):
            here = (lane // reach) == q
            low = jnp.where(here, pltpu.roll(values, (reach * q) % lats, 1), low)
            high = jnp.where(here, pltpu.roll(values, (reach * (q + 1)) % lats, 1), high)
        rim_out[0, part * kf:(part + 1) * kf] = low.astype(BF16)
        rim_out[1, part * kf:(part + 1) * kf] = high.astype(BF16)

    for s in range(2):
        @pl.when(jnp.logical_not(has[s]))
        def _():
            rim_in[s] = jnp.zeros(rim_in.shape[1:], BF16)

    one = jnp.int32(1)
    pl.semaphore_wait(
        barrier, 2 + 3 * jnp.where(has[0], one, 0) + 3 * jnp.where(has[1], one, 0)
    )

    to_west = pltpu.make_async_remote_copy(
        src_ref=own.at[pl.ds(0, body)], dst_ref=east,
        send_sem=send_sem.at[0], recv_sem=recv_sem.at[1],
        device_id=(sides[0], lat), device_id_type=MESH,
    )
    to_east = pltpu.make_async_remote_copy(
        src_ref=own.at[pl.ds(col, body)], dst_ref=west,
        send_sem=send_sem.at[1], recv_sem=recv_sem.at[0],
        device_id=(sides[2], lat), device_id_type=MESH,
    )
    to_west.start()
    to_east.start()

    def rim_copy(s, t):
        return pltpu.make_async_remote_copy(
            src_ref=rim_out.at[s], dst_ref=rim_in.at[1 - s, 2 - t],
            send_sem=rim_send_sem.at[s, t], recv_sem=rim_recv_sem.at[1 - s, 2 - t],
            device_id=(sides[t], lat + 2 * s - 1), device_id_type=MESH,
        )

    for s in range(2):
        @pl.when(has[s])
        def _():
            for t in range(3):
                rim_copy(s, t).start()

    w_fine = w_ref[0] / (kf - 1)
    w_coarse = w_ref[1] / (kc - 1)
    w_paired = w_ref[1] / (kf - 1)
    lat_profile = profile(iota((lats, lats), 0) - iota((lats, lats), 1), reach)
    for d in range(lon_reach + 1):
        taper[d] = lat_profile * (1.0 - 0.75 * (d / lon_reach) * (d / lon_reach))

    block = lons * reach
    shape = (2 * block, lats)
    row, lane = iota(shape, 0), iota(shape, 1)
    side, a_row, i_row = row // block, (row % block) // reach, row % reach
    b_lane, l_lane = lane // reach, lane % reach
    for s in range(2):
        d_lat = i_row - l_lane + reach if s == 0 else reach + l_lane - i_row
        in_lat = jnp.where((side == s) & (b_lane < lons), profile(d_lat, reach), 0.0)
        for t in range(3):
            d_lon = (t - 1) * lons + b_lane - a_row
            n = s * 3 + t
            rim_taper[:, n * lats:(n + 1) * lats] = in_lat * profile(d_lon, lon_reach)

    shape = (2 * lats, lats)
    row, lane = iota(shape, 0), iota(shape, 1)
    place = (row // lats) * halves + (row // reach) % halves
    step = jnp.abs(2 * place - lane // reach)
    weight = jnp.where(step == 0, 1.0, jnp.where(step == 1, 0.5, 0.0))
    weight = jnp.where((row % reach == lane % reach) & (lane < block), weight, 0.0)
    for g in range(groups):
        mine = (row % lats) // (reach * halves) == g
        refine_rim[:, g * lats:(g + 1) * lats] = jnp.where(mine, weight, 0.0).astype(BF16)

    def coarse_parts(refined):
        coarse_anom = refined - jnp.mean(refined, axis=0, keepdims=True)
        pair = refined[:kf]
        return coarse_anom, pair - jnp.mean(pair, axis=0, keepdims=True)

    def set_near(b, fine_anom, refined, vectors):
        coarse_anom, paired = coarse_parts(refined)
        lanes = slice((b + lon_reach) * lats, (b + lon_reach + 1) * lats)
        near[:kf, lanes] = fine_anom
        near[kf:kf + kc, lanes] = coarse_anom.astype(BF16)
        near[kf + kc:, lanes] = paired.astype(BF16)
        near_inc[:, lanes] = vectors
        return coarse_anom, paired

    def set_own(a, refined):
        coarse_anom, paired = set_near(a, fine_own[a], refined, inc_own[a])
        scaled = jnp.concatenate(
            (w_fine * fine_own[a].astype(F32), w_coarse * coarse_anom, -w_paired * paired),
            axis=0,
        )
        own_t[a * lats:(a + 1) * lats] = scaled.T.astype(BF16)

    def add(b, first, last):
        lanes = slice((b + lon_reach) * lats, (b + lon_reach + 1) * lats)
        gram = jnp.dot(
            own_t[first * lats:last * lats], near[:, lanes], preferred_element_type=F32
        )
        tapered = jnp.concatenate(
            [
                (gram[(a - first) * lats:(a - first + 1) * lats] * taper[abs(a - b)]).astype(BF16)
                for a in range(first, last)
            ],
            axis=0,
        )
        acc[:, first * lats:last * lats] += lax.dot_general(
            near_inc[:, lanes], tapered, (((1,), (1,)), ((), ())), preferred_element_type=F32
        )

    acc[...] = jnp.zeros_like(acc)
    for a in range(lon_reach):
        left = coarse_own[a // 2]
        set_own(a, left if a % 2 == 0 else 0.5 * (left + coarse_own[a // 2 + 1]))
    for b in range(lon_reach):
        add(b, 0, lon_reach)

    to_west.wait_recv()
    east_c = [
        east[coarse_at + c * kc:coarse_at + (c + 1) * kc].astype(F32) for c in range(halves)
    ]
    set_own(lon_reach, 0.5 * (coarse_own[halves - 1] + east_c[0]))
    add(lon_reach, 0, lons)
    for b in range(lon_reach):
        add(b, lon_reach, lons)
    for b in range(lon_reach):
        left = east_c[b // 2]
        refined = left if b % 2 == 0 else 0.5 * (left + east_c[b // 2 + 1])
        set_near(
            lons + b, east[b * col:b * col + kf], refined, east[b * col + kf:(b + 1) * col]
        )
        add(lons + b, b + 1, lons)

    to_east.wait_recv()
    west_at = coarse_at - col
    west_c = [
        west[west_at + c * kc:west_at + (c + 1) * kc].astype(F32) for c in range(halves)
    ] + [coarse_own[0]]
    for b in range(1, lons):
        left = west_c[b // 2]
        refined = left if b % 2 == 0 else 0.5 * (left + west_c[b // 2 + 1])
        at = (b - 1) * col if b < lon_reach else body - col
        set_near(b - lons, west[at:at + kf], refined, west[at + kf:at + col])
        add(b - lons, 0, b)

    for s in range(2):
        @pl.when(has[s])
        def _():
            for t in range(3):
                rim_copy(1 - s, 2 - t).wait_recv()

    pairs = []
    for s in range(2):
        for t in range(3):
            pairs.append(
                jnp.concatenate((rim_in[s, t, kf:], rim_in[s, min(t + 1, 2), kf:]), axis=1)
            )
    refined_rim = jnp.dot(
        jnp.concatenate(pairs, axis=0), refine_rim[...], preferred_element_type=F32
    )
    for s in range(2):
        for t in range(3):
            n = s * 3 + t
            lanes = slice(n * lats, (n + 1) * lats)
            refined = jnp.concatenate(
                [
                    refined_rim[n * kf:(n + 1) * kf, g * lats:(g + 1) * lats]
                    for g in range(groups)
                ],
                axis=0,
            )
            coarse_anom, paired = coarse_parts(refined)
            near_rim[:kf, lanes] = rim_in[s, t, :kf]
            near_rim[kf:kf + kc, lanes] = coarse_anom.astype(BF16)
            near_rim[kf + kc:, lanes] = paired.astype(BF16)
            rim_inc[:, lanes] = pltpu.roll(
                rim_in[s, t, :kf].astype(F32), lats - block, 1
            ).astype(BF16)
    own_rim = jnp.concatenate(
        [
            own_t[a * lats + s * (lats - reach):a * lats + s * (lats - reach) + reach]
            for s in range(2)
            for a in range(lons)
        ],
        axis=0,
    )
    gram = jnp.dot(own_rim, near_rim[...], preferred_element_type=F32)
    tapered = (gram * rim_taper[...]).astype(BF16)
    edge = lax.dot_general(
        rim_inc[...], tapered, (((1,), (1,)), ((), ())), preferred_element_type=F32
    )
    lane = iota((nv, lats), 1)
    for a in range(lons):
        low = pltpu.roll(edge, (lats - reach * a) % lats, 1)
        high = pltpu.roll(edge, (2 * lats - reach - block - reach * a) % lats, 1)
        total = acc[:, a * lats:(a + 1) * lats]
        total += jnp.where(lane < reach, low, 0.0) + jnp.where(lane >= lats - reach, high, 0.0)
        out_ref[pl.ds(a, nv, stride=lons), :] = total

    to_west.wait_send()
    to_east.wait_send()
    for s in range(2):
        @pl.when(has[s])
        def _():
            for t in range(3):
                rim_copy(s, t).wait_send()


def solution(mesh):
    n_lon, n_lat = mesh.shape["lon"], mesh.shape["lat"]

    def per_device(fine, coarse, inc, weights):
        kf, lons, lats = fine.shape
        kc, halves, _ = coarse.shape
        nv = inc.shape[0]
        members, col, near_lons = 2 * kf + kc, kf + nv, 3 * lons - 2
        body = (lons - 1) * col + halves * kc
        assert nv == kf and 2 * lons * (lats // 8) == lats and kc * halves == 2 * lons * kf
        result = pl.pallas_call(
            functools.partial(kernel, (n_lon, n_lat, kf, kc, nv, lons, lats)),
            out_shape=jax.ShapeDtypeStruct((nv * lons, lats), F32),
            in_specs=[pl.BlockSpec(memory_space=pltpu.SMEM)]
            + [pl.BlockSpec(memory_space=pl.ANY)] * 3,
            out_specs=pl.BlockSpec(memory_space=pltpu.VMEM),
            scratch_shapes=[
                pltpu.VMEM((kf * lons, lats), BF16),
                pltpu.VMEM((kc * halves, lats), BF16),
                pltpu.VMEM((nv * lons, lats), BF16),
                pltpu.VMEM((col * lons + kc * halves, lats), F32),
                pltpu.VMEM((body + col, lats), BF16),
                pltpu.VMEM((body, lats), BF16),
                pltpu.VMEM((body, lats), BF16),
                pltpu.VMEM((2, 2 * kf, lats), BF16),
                pltpu.VMEM((2, 3, 2 * kf, lats), BF16),
                pltpu.VMEM((members, near_lons * lats), BF16),
                pltpu.VMEM((nv, near_lons * lats), BF16),
                pltpu.VMEM((lons * lats, members), BF16),
                pltpu.VMEM((members, 6 * lats), BF16),
                pltpu.VMEM((nv, 6 * lats), BF16),
                pltpu.VMEM((lons, lats, lats), F32),
                pltpu.VMEM((lats, 6 * lats), F32),
                pltpu.VMEM((2 * lats, (kc // kf) * lats), BF16),
                pltpu.VMEM((nv, lons * lats), F32),
                pltpu.SemaphoreType.DMA((3,)),
                pltpu.SemaphoreType.DMA((2,)),
                pltpu.SemaphoreType.DMA((2,)),
                pltpu.SemaphoreType.DMA((2, 3)),
                pltpu.SemaphoreType.DMA((2, 3)),
            ],
            compiler_params=pltpu.CompilerParams(collective_id=0, has_side_effects=True),
            name="covariance",
        )(
            weights,
            fine.reshape(kf * lons, lats),
            coarse.reshape(kc * halves, lats),
            inc.reshape(nv * lons, lats),
        )
        return result.reshape(nv, lons, lats)

    spec = P(None, "lon", "lat")
    return jax.shard_map(
        per_device, mesh=mesh, in_specs=(spec, spec, spec, P()), out_specs=spec, check_vma=False
    )
```

```python
import functools

import jax
import jax.numpy as jnp
from jax import lax
from jax.experimental import pallas as pl
from jax.experimental.pallas import tpu as pltpu
from jax.sharding import PartitionSpec as P

MESH = pl.DeviceIdType.MESH
F32, BF16 = jnp.float32, jnp.bfloat16


def profile(distance, extent):
    ratio = distance.astype(F32) / extent
    return jnp.where(jnp.abs(distance) <= extent, 1.0 - 0.75 * ratio * ratio, 0.0)


def iota(shape, dim):
    return lax.broadcasted_iota(jnp.int32, shape, dim)


def kernel(
    sizes, weights_ref, fine_ref, coarse_ref, inc_ref, out_ref,
    w_ref, fine_in, coarse_in, inc_in, wide, own, own_c, west, east, west_cin, east_cin, rim_out, rim_in,
    near, near_inc, own_t, near_rim, rim_inc, taper, rim_taper, refine_rim, acc,
    in_sem, send_sem, recv_sem, rim_send_sem, rim_recv_sem,
):
    n_lon, n_lat, kf, kc, nv, lons, lats = sizes
    halves, reach, lon_reach = lons // 2, lats // 8, lons - 1
    col = kf + nv
    groups = kc // kf
    body = lon_reach * col
    ratio = (kc - 1) / (kf - 1)
    lon, lat = lax.axis_index("lon"), lax.axis_index("lat")
    sides = (lax.rem(lon + n_lon - 1, n_lon), lon, lax.rem(lon + 1, n_lon))
    has = (lat > 0, lat < n_lat - 1)

    barrier = pltpu.get_barrier_semaphore()

    def greet(to_lon, to_lat):
        pl.semaphore_signal(barrier, inc=1, device_id=(to_lon, to_lat), device_id_type=MESH)

    greet(sides[0], lat)
    greet(sides[2], lat)
    for s in range(2):
        @pl.when(has[s])
        def _():
            for t in range(3):
                greet(sides[t], lat + 2 * s - 1)

    loads = [
        pltpu.make_async_copy(src, dst, in_sem.at[n])
        for n, (src, dst) in enumerate(
            ((fine_ref, fine_in), (coarse_ref, coarse_in), (inc_ref, inc_in), (weights_ref, w_ref))
        )
    ]
    for load in loads:
        load.start()

    f_at, c_at, i_at = 0, kf * lons, kf * lons + kc * halves

    loads[0].wait()
    wide[f_at:f_at + kf * lons] = fine_in[...].astype(F32)
    loads[1].wait()
    wide[c_at:c_at + kc * halves] = coarse_in[...].astype(F32)
    loads[2].wait()
    wide[i_at:i_at + nv * lons] = inc_in[...].astype(F32)

    fine_own, inc_own, coarse_own = [], [], []
    for a in range(lons):
        values = wide[pl.ds(f_at + a, kf, stride=lons), :]
        anom = (values - jnp.mean(values, axis=0, keepdims=True)).astype(BF16)
        vectors = wide[pl.ds(i_at + a, nv, stride=lons), :].astype(BF16)
        at = a * col
        own[at:at + kf] = anom
        own[at + kf:at + col] = vectors
        fine_own.append(anom)
        inc_own.append(vectors)
    for c in range(halves):
        values = wide[pl.ds(c_at + c, kc, stride=halves), :]
        own_c[c * kc:(c + 1) * kc] = values.astype(BF16)
        coarse_own.append(values)

    lane = iota((kf, lats), 1)
    packs = (
        [v.astype(F32) for v in fine_own] + [v.astype(F32) for v in inc_own],
        [coarse_own[c][g * kf:(g + 1) * kf] for g in range(groups) for c in range(halves)],
    )
    for part in range(2):
        low = high = jnp.zeros((kf, lats), F32)
        for q, values in enumerate(packs[part]):
            here = (lane // reach) == q
            low = jnp.where(here, pltpu.roll(values, (reach * q) % lats, 1), low)
            high = jnp.where(here, pltpu.roll(values, (reach * (q + 1)) % lats, 1), high)
        rim_out[0, part * kf:(part + 1) * kf] = low.astype(BF16)
        rim_out[1, part * kf:(part + 1) * kf] = high.astype(BF16)

    for s in range(2):
        @pl.when(jnp.logical_not(has[s]))
        def _():
            rim_in[s] = jnp.zeros(rim_in.shape[1:], BF16)

    one = jnp.int32(1)
    pl.semaphore_wait(
        barrier, 2 + 3 * jnp.where(has[0], one, 0) + 3 * jnp.where(has[1], one, 0)
    )

    def send(src, dst, n, towards):
        return pltpu.make_async_remote_copy(
            src_ref=src, dst_ref=dst, send_sem=send_sem.at[n], recv_sem=recv_sem.at[n],
            device_id=(sides[towards], lat), device_id_type=MESH,
        )

    coarse_west = send(own_c, east_cin, 0, 0)
    coarse_east = send(own_c, west_cin, 1, 2)
    rest_west = send(own.at[pl.ds(0, body)], east, 2, 0)
    rest_east = send(own.at[pl.ds(col, body)], west, 3, 2)
    coarse_west.start()
    coarse_east.start()

    def rim_copy(s, t):
        return pltpu.make_async_remote_copy(
            src_ref=rim_out.at[s], dst_ref=rim_in.at[1 - s, 2 - t],
            send_sem=rim_send_sem.at[s, t], recv_sem=rim_recv_sem.at[1 - s, 2 - t],
            device_id=(sides[t], lat + 2 * s - 1), device_id_type=MESH,
        )

    for s in range(2):
        @pl.when(has[s])
        def _():
            for t in (0, 2, 1):
                rim_copy(s, t).start()

    rest_west.start()
    rest_east.start()

    loads[3].wait()
    w_coarse = w_ref[1] / (kc - 1)
    fine_ratio = ratio * w_ref[0] / w_ref[1]
    lat_profile = w_coarse * profile(iota((lats, lats), 0) - iota((lats, lats), 1), reach)
    for d in range(lon_reach + 1):
        taper[d] = lat_profile * (1.0 - 0.75 * (d / lon_reach) * (d / lon_reach))

    block = lons * reach
    shape = (2 * block, lats)
    row, lane = iota(shape, 0), iota(shape, 1)
    side, a_row, i_row = row // block, (row % block) // reach, row % reach
    b_lane, l_lane = lane // reach, lane % reach
    for s in range(2):
        d_lat = i_row - l_lane + reach if s == 0 else reach + l_lane - i_row
        in_lat = jnp.where((side == s) & (b_lane < lons), w_coarse * profile(d_lat, reach), 0.0)
        for t in range(3):
            d_lon = (t - 1) * lons + b_lane - a_row
            n = s * 3 + t
            rim_taper[:, n * lats:(n + 1) * lats] = in_lat * profile(d_lon, lon_reach)

    shape = (2 * lats, lats)
    row, lane = iota(shape, 0), iota(shape, 1)
    place = (row // lats) * halves + (row // reach) % halves
    step = jnp.abs(2 * place - lane // reach)
    weight = jnp.where(step == 0, 1.0, jnp.where(step == 1, 0.5, 0.0))
    weight = jnp.where((row % reach == lane % reach) & (lane < block), weight, 0.0)
    for g in range(groups):
        mine = (row % lats) // (reach * halves) == g
        refine_rim[:, g * lats:(g + 1) * lats] = jnp.where(mine, weight, 0.0).astype(BF16)

    def coarse_parts(refined):
        coarse_anom = refined - jnp.mean(refined, axis=0, keepdims=True)
        pair = refined[:kf]
        paired = pair - jnp.mean(pair, axis=0, keepdims=True)
        return coarse_anom.astype(BF16), paired.astype(BF16)

    def lanes_of(b):
        return slice((b + lon_reach) * lats, (b + lon_reach + 1) * lats)

    def set_near(to, lanes, refined):
        coarse_anom, paired = coarse_parts(refined)
        to[2 * kf:2 * kf + kc, lanes] = coarse_anom
        to[2 * kf + kc:3 * kf + kc, lanes] = paired
        to[3 * kf + kc:, lanes] = paired
        return coarse_anom, paired

    def set_fine(b, fine_anom, vectors):
        near[:kf, lanes_of(b)] = fine_anom
        near[kf:2 * kf, lanes_of(b)] = fine_anom
        near_inc[:, lanes_of(b)] = vectors

    def split(scale, values):
        scaled = scale * values.astype(F32)
        high = scaled.astype(BF16).astype(F32)
        return [high, scaled - high]

    def set_own(a, refined):
        coarse_anom, paired = set_near(near, lanes_of(a), refined)
        set_fine(a, fine_own[a], inc_own[a])
        parts = split(fine_ratio, fine_own[a]) + [coarse_anom.astype(F32)] + split(-ratio, paired)
        own_t[a * lats:(a + 1) * lats] = jnp.concatenate(parts, axis=0).T.astype(BF16)

    def add(b, first, last):
        lanes = lanes_of(b)
        gram = jnp.dot(
            own_t[first * lats:last * lats], near[:, lanes], preferred_element_type=F32
        )
        tapered = jnp.concatenate(
            [
                (gram[(a - first) * lats:(a - first + 1) * lats] * taper[abs(a - b)]).astype(BF16)
                for a in range(first, last)
            ],
            axis=0,
        )
        acc[:, first * lats:last * lats] += lax.dot_general(
            near_inc[:, lanes], tapered, (((1,), (1,)), ((), ())), preferred_element_type=F32
        )

    acc[...] = jnp.zeros_like(acc)
    for a in range(lon_reach):
        left = coarse_own[a // 2]
        set_own(a, left if a % 2 == 0 else 0.5 * (left + coarse_own[a // 2 + 1]))
    for b in range(lon_reach):
        add(b, 0, lon_reach)

    def from_east():
        coarse_west.wait_recv()
        east_c = [east_cin[c * kc:(c + 1) * kc].astype(F32) for c in range(halves)]
        set_own(lon_reach, 0.5 * (coarse_own[halves - 1] + east_c[0]))
        add(lon_reach, 0, lons)
        for b in range(lon_reach):
            add(b, lon_reach, lons)
        for b in range(lon_reach):
            left = east_c[b // 2]
            refined = left if b % 2 == 0 else 0.5 * (left + east_c[b // 2 + 1])
            set_near(near, lanes_of(lons + b), refined)
        rest_west.wait_recv()
        for b in range(lon_reach):
            at = b * col
            set_fine(lons + b, east[at:at + kf], east[at + kf:at + col])
            add(lons + b, b + 1, lons)

    def from_west():
        coarse_east.wait_recv()
        west_c = [west_cin[c * kc:(c + 1) * kc].astype(F32) for c in range(halves)]
        west_c.append(coarse_own[0])
        for b in range(1, lons):
            left = west_c[b // 2]
            refined = left if b % 2 == 0 else 0.5 * (left + west_c[b // 2 + 1])
            set_near(near, lanes_of(b - lons), refined)
        rest_east.wait_recv()
        for b in range(1, lons):
            at = (b - 1) * col
            set_fine(b - lons, west[at:at + kf], west[at + kf:at + col])
            add(b - lons, 0, b)

    is_last = lon == n_lon - 1
    pl.when(jnp.logical_not(is_last))(from_east)
    from_west()
    pl.when(is_last)(from_east)

    for s in range(2):
        @pl.when(has[s])
        def _():
            for t in range(3):
                rim_copy(1 - s, 2 - t).wait_recv()

    pairs = []
    for s in range(2):
        for t in range(3):
            pairs.append(
                jnp.concatenate((rim_in[s, t, kf:], rim_in[s, min(t + 1, 2), kf:]), axis=1)
            )
    refined_rim = jnp.dot(
        jnp.concatenate(pairs, axis=0), refine_rim[...], preferred_element_type=F32
    )
    for s in range(2):
        for t in range(3):
            n = s * 3 + t
            lanes = slice(n * lats, (n + 1) * lats)
            refined = jnp.concatenate(
                [
                    refined_rim[n * kf:(n + 1) * kf, g * lats:(g + 1) * lats]
                    for g in range(groups)
                ],
                axis=0,
            )
            set_near(near_rim, lanes, refined)
            near_rim[:kf, lanes] = rim_in[s, t, :kf]
            near_rim[kf:2 * kf, lanes] = rim_in[s, t, :kf]
            rim_inc[:, lanes] = pltpu.roll(
                rim_in[s, t, :kf].astype(F32), lats - block, 1
            ).astype(BF16)
    own_rim = jnp.concatenate(
        [
            own_t[a * lats + s * (lats - reach):a * lats + s * (lats - reach) + reach]
            for s in range(2)
            for a in range(lons)
        ],
        axis=0,
    )
    gram = jnp.dot(own_rim, near_rim[...], preferred_element_type=F32)
    tapered = (gram * rim_taper[...]).astype(BF16)
    edge = lax.dot_general(
        rim_inc[...], tapered, (((1,), (1,)), ((), ())), preferred_element_type=F32
    )
    lane = iota((nv, lats), 1)
    for a in range(lons):
        low = pltpu.roll(edge, (lats - reach * a) % lats, 1)
        high = pltpu.roll(edge, (2 * lats - reach - block - reach * a) % lats, 1)
        total = acc[:, a * lats:(a + 1) * lats]
        total += jnp.where(lane < reach, low, 0.0) + jnp.where(lane >= lats - reach, high, 0.0)
        out_ref[pl.ds(a, nv, stride=lons), :] = total

    for copy in (coarse_west, coarse_east, rest_west, rest_east):
        copy.wait_send()
    for s in range(2):
        @pl.when(has[s])
        def _():
            for t in range(3):
                rim_copy(s, t).wait_send()


def solution(mesh):
    n_lon, n_lat = mesh.shape["lon"], mesh.shape["lat"]

    def per_device(fine, coarse, inc, weights):
        kf, lons, lats = fine.shape
        kc, halves, _ = coarse.shape
        nv = inc.shape[0]
        members, col, near_lons = 4 * kf + kc, kf + nv, 3 * lons - 2
        body = (lons - 1) * col
        assert nv == kf and 2 * lons * (lats // 8) == lats and kc * halves == 2 * lons * kf
        result = pl.pallas_call(
            functools.partial(kernel, (n_lon, n_lat, kf, kc, nv, lons, lats)),
            out_shape=pltpu.VMEM((nv * lons, lats), F32),
            in_specs=[pl.BlockSpec(memory_space=pl.ANY)] * 4,
            out_specs=pl.BlockSpec(memory_space=pltpu.VMEM),
            scratch_shapes=[
                pltpu.SMEM(weights.shape, F32),
                pltpu.VMEM((kf * lons, lats), BF16),
                pltpu.VMEM((kc * halves, lats), BF16),
                pltpu.VMEM((nv * lons, lats), BF16),
                pltpu.VMEM((col * lons + kc * halves, lats), F32),
                pltpu.VMEM((body + col, lats), BF16),
                pltpu.VMEM((kc * halves, lats), BF16),
                pltpu.VMEM((body, lats), BF16),
                pltpu.VMEM((body, lats), BF16),
                pltpu.VMEM((kc * halves, lats), BF16),
                pltpu.VMEM((kc * halves, lats), BF16),
                pltpu.VMEM((2, 2 * kf, lats), BF16),
                pltpu.VMEM((2, 3, 2 * kf, lats), BF16),
                pltpu.VMEM((members, near_lons * lats), BF16),
                pltpu.VMEM((nv, near_lons * lats), BF16),
                pltpu.VMEM((lons * lats, members), BF16),
                pltpu.VMEM((members, 6 * lats), BF16),
                pltpu.VMEM((nv, 6 * lats), BF16),
                pltpu.VMEM((lons, lats, lats), F32),
                pltpu.VMEM((lats, 6 * lats), F32),
                pltpu.VMEM((2 * lats, (kc // kf) * lats), BF16),
                pltpu.VMEM((nv, lons * lats), F32),
                pltpu.SemaphoreType.DMA((4,)),
                pltpu.SemaphoreType.DMA((4,)),
                pltpu.SemaphoreType.DMA((4,)),
                pltpu.SemaphoreType.DMA((2, 3)),
                pltpu.SemaphoreType.DMA((2, 3)),
            ],
            compiler_params=pltpu.CompilerParams(collective_id=0, has_side_effects=True),
            name="covariance",
        )(
            weights,
            fine.reshape(kf * lons, lats),
            coarse.reshape(kc * halves, lats),
            inc.reshape(nv * lons, lats),
        )
        return result.reshape(nv, lons, lats)

    spec = P(None, "lon", "lat")
    return jax.shard_map(
        per_device, mesh=mesh, in_specs=(spec, spec, spec, P()), out_specs=spec, check_vma=False
    )
```

```python
import functools

import jax
import jax.numpy as jnp
from jax import lax
from jax.experimental import pallas as pl
from jax.experimental.pallas import tpu as pltpu
from jax.sharding import PartitionSpec as P

MESH = pl.DeviceIdType.MESH
F32, BF16 = jnp.float32, jnp.bfloat16


def profile(distance, extent):
    ratio = distance.astype(F32) / extent
    return jnp.where(jnp.abs(distance) <= extent, 1.0 - 0.75 * ratio * ratio, 0.0)


def iota(shape, dim):
    return lax.broadcasted_iota(jnp.int32, shape, dim)


def kernel(
    sizes, weights_ref, fine_ref, coarse_ref, inc_ref, out_ref,
    w_ref, fine_in, coarse_in, inc_in, wide, own, own_c, west, east, west_cin, east_cin, rim_out, rim_in,
    near, near_inc, own_t, near_rim, rim_inc, taper, rim_taper, refine_rim, acc,
    in_sem, send_sem, recv_sem, rim_send_sem, rim_recv_sem,
):
    n_lon, n_lat, kf, kc, nv, lons, lats = sizes
    halves, reach, lon_reach = lons // 2, lats // 8, lons - 1
    col = kf + nv
    groups = kc // kf
    body = lon_reach * col
    ratio = (kc - 1) / (kf - 1)
    lon, lat = lax.axis_index("lon"), lax.axis_index("lat")
    sides = (lax.rem(lon + n_lon - 1, n_lon), lon, lax.rem(lon + 1, n_lon))
    has = (lat > 0, lat < n_lat - 1)

    loads = [
        pltpu.make_async_copy(src, dst, in_sem.at[n])
        for n, (src, dst) in enumerate(
            ((coarse_ref, coarse_in), (fine_ref, fine_in), (inc_ref, inc_in), (weights_ref, w_ref))
        )
    ]
    for load in loads:
        load.start()

    barrier = pltpu.get_barrier_semaphore()

    def greet(to_lon, to_lat):
        pl.semaphore_signal(barrier, inc=1, device_id=(to_lon, to_lat), device_id_type=MESH)

    greet(sides[0], lat)
    greet(sides[2], lat)
    for s in range(2):
        @pl.when(has[s])
        def _():
            for t in range(3):
                greet(sides[t], lat + 2 * s - 1)

    f_at, c_at, i_at = 0, kf * lons, kf * lons + kc * halves
    loads[0].wait()
    wide[c_at:c_at + kc * halves] = coarse_in[...].astype(F32)
    coarse_own = []
    for c in range(halves):
        values = wide[pl.ds(c_at + c, kc, stride=halves), :]
        own_c[c * kc:(c + 1) * kc] = values.astype(BF16)
        coarse_own.append(values)

    for s in range(2):
        @pl.when(jnp.logical_not(has[s]))
        def _():
            rim_in[s] = jnp.zeros(rim_in.shape[1:], BF16)

    one = jnp.int32(1)
    pl.semaphore_wait(
        barrier, 2 + 3 * jnp.where(has[0], one, 0) + 3 * jnp.where(has[1], one, 0)
    )

    def send(src, dst, n, towards):
        return pltpu.make_async_remote_copy(
            src_ref=src, dst_ref=dst, send_sem=send_sem.at[n], recv_sem=recv_sem.at[n],
            device_id=(sides[towards], lat), device_id_type=MESH,
        )

    coarse_west = send(own_c, east_cin, 0, 0)
    coarse_east = send(own_c, west_cin, 1, 2)
    rest_west = send(own.at[pl.ds(0, body)], east, 2, 0)
    rest_east = send(own.at[pl.ds(col, body)], west, 3, 2)
    coarse_west.start()
    coarse_east.start()

    fine_own, inc_own = [], []
    loads[1].wait()
    wide[f_at:f_at + kf * lons] = fine_in[...].astype(F32)
    for a in range(lons):
        values = wide[pl.ds(f_at + a, kf, stride=lons), :]
        anom = (values - jnp.mean(values, axis=0, keepdims=True)).astype(BF16)
        own[a * col:a * col + kf] = anom
        fine_own.append(anom)
    loads[2].wait()
    wide[i_at:i_at + nv * lons] = inc_in[...].astype(F32)
    for a in range(lons):
        vectors = wide[pl.ds(i_at + a, nv, stride=lons), :].astype(BF16)
        own[a * col + kf:(a + 1) * col] = vectors
        inc_own.append(vectors)

    lane = iota((kf, lats), 1)
    packs = (
        [v.astype(F32) for v in fine_own] + [v.astype(F32) for v in inc_own],
        [coarse_own[c][g * kf:(g + 1) * kf] for g in range(groups) for c in range(halves)],
    )
    for part in range(2):
        low = high = jnp.zeros((kf, lats), F32)
        for q, values in enumerate(packs[part]):
            here = (lane // reach) == q
            low = jnp.where(here, pltpu.roll(values, (reach * q) % lats, 1), low)
            high = jnp.where(here, pltpu.roll(values, (reach * (q + 1)) % lats, 1), high)
        rim_out[0, part * kf:(part + 1) * kf] = low.astype(BF16)
        rim_out[1, part * kf:(part + 1) * kf] = high.astype(BF16)

    def rim_copy(s, t):
        return pltpu.make_async_remote_copy(
            src_ref=rim_out.at[s], dst_ref=rim_in.at[1 - s, 2 - t],
            send_sem=rim_send_sem.at[s, t], recv_sem=rim_recv_sem.at[1 - s, 2 - t],
            device_id=(sides[t], lat + 2 * s - 1), device_id_type=MESH,
        )

    for s in range(2):
        @pl.when(has[s])
        def _():
            for t in (0, 2, 1):
                rim_copy(s, t).start()

    rest_west.start()
    rest_east.start()

    loads[3].wait()
    w_coarse = w_ref[1] / (kc - 1)
    fine_ratio = ratio * w_ref[0] / w_ref[1]
    lat_profile = w_coarse * profile(iota((lats, lats), 0) - iota((lats, lats), 1), reach)
    for d in range(lon_reach + 1):
        taper[d] = lat_profile * (1.0 - 0.75 * (d / lon_reach) * (d / lon_reach))

    block = lons * reach
    shape = (2 * block, lats)
    row, lane = iota(shape, 0), iota(shape, 1)
    side, a_row, i_row = row // block, (row % block) // reach, row % reach
    b_lane, l_lane = lane // reach, lane % reach
    for s in range(2):
        d_lat = i_row - l_lane + reach if s == 0 else reach + l_lane - i_row
        in_lat = jnp.where((side == s) & (b_lane < lons), w_coarse * profile(d_lat, reach), 0.0)
        for t in range(3):
            d_lon = (t - 1) * lons + b_lane - a_row
            n = 2 * t + s
            rim_taper[:, n * lats:(n + 1) * lats] = in_lat * profile(d_lon, lon_reach)

    shape = (2 * lats, lats)
    row, lane = iota(shape, 0), iota(shape, 1)
    place = (row // lats) * halves + (row // reach) % halves
    step = jnp.abs(2 * place - lane // reach)
    weight = jnp.where(step == 0, 1.0, jnp.where(step == 1, 0.5, 0.0))
    weight = jnp.where((row % reach == lane % reach) & (lane < block), weight, 0.0)
    for g in range(groups):
        mine = (row % lats) // (reach * halves) == g
        refine_rim[:, g * lats:(g + 1) * lats] = jnp.where(mine, weight, 0.0).astype(BF16)

    def coarse_parts(refined):
        coarse_anom = refined - jnp.mean(refined, axis=0, keepdims=True)
        pair = refined[:kf]
        paired = pair - jnp.mean(pair, axis=0, keepdims=True)
        return coarse_anom.astype(BF16), paired.astype(BF16)

    def lanes_of(b):
        return slice((b + lon_reach) * lats, (b + lon_reach + 1) * lats)

    def set_near(to, lanes, refined):
        coarse_anom, paired = coarse_parts(refined)
        to[2 * kf:2 * kf + kc, lanes] = coarse_anom
        to[2 * kf + kc:3 * kf + kc, lanes] = paired
        to[3 * kf + kc:, lanes] = paired
        return coarse_anom, paired

    def set_fine(b, fine_anom, vectors):
        near[:kf, lanes_of(b)] = fine_anom
        near[kf:2 * kf, lanes_of(b)] = fine_anom
        near_inc[:, lanes_of(b)] = vectors

    def split(scale, values):
        scaled = scale * values.astype(F32)
        high = scaled.astype(BF16).astype(F32)
        return [high, scaled - high]

    def set_own(a, refined):
        coarse_anom, paired = set_near(near, lanes_of(a), refined)
        set_fine(a, fine_own[a], inc_own[a])
        parts = split(fine_ratio, fine_own[a]) + [coarse_anom.astype(F32)] + split(-ratio, paired)
        own_t[a * lats:(a + 1) * lats] = jnp.concatenate(parts, axis=0).T.astype(BF16)

    def add(b, first, last):
        lanes = lanes_of(b)
        gram = jnp.dot(
            own_t[first * lats:last * lats], near[:, lanes], preferred_element_type=F32
        )
        tapered = jnp.concatenate(
            [
                (gram[(a - first) * lats:(a - first + 1) * lats] * taper[abs(a - b)]).astype(BF16)
                for a in range(first, last)
            ],
            axis=0,
        )
        acc[:, first * lats:last * lats] += lax.dot_general(
            near_inc[:, lanes], tapered, (((1,), (1,)), ((), ())), preferred_element_type=F32
        )

    acc[...] = jnp.zeros_like(acc)
    for a in range(lon_reach):
        left = coarse_own[a // 2]
        set_own(a, left if a % 2 == 0 else 0.5 * (left + coarse_own[a // 2 + 1]))
    for b in range(lon_reach):
        add(b, 0, lon_reach)

    def rim_pack(s, t):
        return jnp.concatenate((rim_in[s, t, kf:], rim_in[s, min(t + 1, 2), kf:]), axis=1)

    def wait_rims(some):
        for s in range(2):
            @pl.when(has[s])
            def _():
                for t in some:
                    rim_copy(1 - s, 2 - t).wait_recv()

    def set_rims(some):
        order = [(s, t) for s in range(2) for t in some]
        refined_rim = jnp.dot(
            jnp.concatenate([rim_pack(s, t) for s, t in order], axis=0),
            refine_rim[...],
            preferred_element_type=F32,
        )
        for n, (s, t) in enumerate(order):
            lanes = slice((2 * t + s) * lats, (2 * t + s + 1) * lats)
            refined = jnp.concatenate(
                [
                    refined_rim[n * kf:(n + 1) * kf, g * lats:(g + 1) * lats]
                    for g in range(groups)
                ],
                axis=0,
            )
            set_near(near_rim, lanes, refined)
            near_rim[:kf, lanes] = rim_in[s, t, :kf]
            near_rim[kf:2 * kf, lanes] = rim_in[s, t, :kf]
            rim_inc[:, lanes] = pltpu.roll(
                rim_in[s, t, :kf].astype(F32), lats - block, 1
            ).astype(BF16)

    def rim_product(first, last):
        lanes = slice(2 * first * lats, 2 * last * lats)
        gram = jnp.dot(own_rim, near_rim[:, lanes], preferred_element_type=F32)
        tapered = (gram * rim_taper[:, lanes]).astype(BF16)
        return lax.dot_general(
            rim_inc[:, lanes], tapered, (((1,), (1,)), ((), ())), preferred_element_type=F32
        )

    coarse_west.wait_recv()
    east_c = [east_cin[c * kc:(c + 1) * kc].astype(F32) for c in range(halves)]
    set_own(lon_reach, 0.5 * (coarse_own[halves - 1] + east_c[0]))
    add(lon_reach, 0, lons)
    for b in range(lon_reach):
        add(b, lon_reach, lons)
    for b in range(lon_reach):
        left = east_c[b // 2]
        refined = left if b % 2 == 0 else 0.5 * (left + east_c[b // 2 + 1])
        set_near(near, lanes_of(lons + b), refined)
    own_rim = jnp.concatenate(
        [
            own_t[a * lats + s * (lats - reach):a * lats + s * (lats - reach) + reach]
            for s in range(2)
            for a in range(lons)
        ],
        axis=0,
    )

    coarse_east.wait_recv()
    west_c = [west_cin[c * kc:(c + 1) * kc].astype(F32) for c in range(halves)]
    west_c.append(coarse_own[0])
    for b in range(1, lons):
        left = west_c[b // 2]
        refined = left if b % 2 == 0 else 0.5 * (left + west_c[b // 2 + 1])
        set_near(near, lanes_of(b - lons), refined)

    rest_west.wait_recv()
    wait_rims((1, 2))
    for b in range(lon_reach):
        at = b * col
        set_fine(lons + b, east[at:at + kf], east[at + kf:at + col])
        add(lons + b, b + 1, lons)
    set_rims((1, 2))
    edge = rim_product(1, 3)

    rest_east.wait_recv()
    wait_rims((0,))
    for b in range(1, lons):
        at = (b - 1) * col
        set_fine(b - lons, west[at:at + kf], west[at + kf:at + col])
        add(b - lons, 0, b)
    set_rims((0,))
    edge += rim_product(0, 1)

    lane = iota((nv, lats), 1)
    for a in range(lons):
        low = pltpu.roll(edge, (lats - reach * a) % lats, 1)
        high = pltpu.roll(edge, (2 * lats - reach - block - reach * a) % lats, 1)
        total = acc[:, a * lats:(a + 1) * lats]
        total += jnp.where(lane < reach, low, 0.0) + jnp.where(lane >= lats - reach, high, 0.0)
        out_ref[pl.ds(a, nv, stride=lons), :] = total

    for copy in (coarse_west, coarse_east, rest_west, rest_east):
        copy.wait_send()
    for s in range(2):
        @pl.when(has[s])
        def _():
            for t in range(3):
                rim_copy(s, t).wait_send()


def solution(mesh):
    n_lon, n_lat = mesh.shape["lon"], mesh.shape["lat"]

    def per_device(fine, coarse, inc, weights):
        kf, lons, lats = fine.shape
        kc, halves, _ = coarse.shape
        nv = inc.shape[0]
        members, col, near_lons = 4 * kf + kc, kf + nv, 3 * lons - 2
        body = (lons - 1) * col
        assert nv == kf and 2 * lons * (lats // 8) == lats and kc * halves == 2 * lons * kf
        result = pl.pallas_call(
            functools.partial(kernel, (n_lon, n_lat, kf, kc, nv, lons, lats)),
            out_shape=pltpu.VMEM((nv * lons, lats), F32),
            in_specs=[pl.BlockSpec(memory_space=pl.ANY)] * 4,
            out_specs=pl.BlockSpec(memory_space=pltpu.VMEM),
            scratch_shapes=[
                pltpu.SMEM(weights.shape, F32),
                pltpu.VMEM((kf * lons, lats), BF16),
                pltpu.VMEM((kc * halves, lats), BF16),
                pltpu.VMEM((nv * lons, lats), BF16),
                pltpu.VMEM((col * lons + kc * halves, lats), F32),
                pltpu.VMEM((body + col, lats), BF16),
                pltpu.VMEM((kc * halves, lats), BF16),
                pltpu.VMEM((body, lats), BF16),
                pltpu.VMEM((body, lats), BF16),
                pltpu.VMEM((kc * halves, lats), BF16),
                pltpu.VMEM((kc * halves, lats), BF16),
                pltpu.VMEM((2, 2 * kf, lats), BF16),
                pltpu.VMEM((2, 3, 2 * kf, lats), BF16),
                pltpu.VMEM((members, near_lons * lats), BF16),
                pltpu.VMEM((nv, near_lons * lats), BF16),
                pltpu.VMEM((lons * lats, members), BF16),
                pltpu.VMEM((members, 6 * lats), BF16),
                pltpu.VMEM((nv, 6 * lats), BF16),
                pltpu.VMEM((lons, lats, lats), F32),
                pltpu.VMEM((lats, 6 * lats), F32),
                pltpu.VMEM((2 * lats, (kc // kf) * lats), BF16),
                pltpu.VMEM((nv, lons * lats), F32),
                pltpu.SemaphoreType.DMA((4,)),
                pltpu.SemaphoreType.DMA((4,)),
                pltpu.SemaphoreType.DMA((4,)),
                pltpu.SemaphoreType.DMA((2, 3)),
                pltpu.SemaphoreType.DMA((2, 3)),
            ],
            compiler_params=pltpu.CompilerParams(collective_id=0, has_side_effects=True),
            name="covariance",
        )(
            weights,
            fine.reshape(kf * lons, lats),
            coarse.reshape(kc * halves, lats),
            inc.reshape(nv * lons, lats),
        )
        return result.reshape(nv, lons, lats)

    spec = P(None, "lon", "lat")
    return jax.shard_map(
        per_device, mesh=mesh, in_specs=(spec, spec, spec, P()), out_specs=spec, check_vma=False
    )
```

```python
import functools

import jax
import jax.numpy as jnp
from jax import lax
from jax.experimental import pallas as pl
from jax.experimental.pallas import tpu as pltpu
from jax.sharding import PartitionSpec as P

MESH = pl.DeviceIdType.MESH
F32, BF16 = jnp.float32, jnp.bfloat16


def profile(distance, extent):
    ratio = distance.astype(F32) / extent
    return jnp.where(jnp.abs(distance) <= extent, 1.0 - 0.75 * ratio * ratio, 0.0)


def iota(shape, dim):
    return lax.broadcasted_iota(jnp.int32, shape, dim)


def kernel(
    sizes, weights_ref, fine_ref, coarse_ref, inc_ref, out_ref,
    w_ref, fine_in, coarse_in, inc_in, wide, own, own_c, west, east, west_cin, east_cin, rim_out, rim_in,
    near, near_inc, own_t, near_rim, rim_inc, taper, rim_taper, refine_rim, acc,
    in_sem, send_sem, recv_sem, rim_send_sem, rim_recv_sem,
):
    n_lon, n_lat, kf, kc, nv, lons, lats = sizes
    halves, reach, lon_reach = lons // 2, lats // 8, lons - 1
    col = kf + nv
    groups = kc // kf
    body = lon_reach * col
    ratio = (kc - 1) / (kf - 1)
    lon, lat = lax.axis_index("lon"), lax.axis_index("lat")
    sides = (lax.rem(lon + n_lon - 1, n_lon), lon, lax.rem(lon + 1, n_lon))
    has = (lat > 0, lat < n_lat - 1)

    loads = [
        pltpu.make_async_copy(src, dst, in_sem.at[n])
        for n, (src, dst) in enumerate(
            ((coarse_ref, coarse_in), (fine_ref, fine_in), (inc_ref, inc_in), (weights_ref, w_ref))
        )
    ]
    for load in loads:
        load.start()

    barrier = pltpu.get_barrier_semaphore()

    def greet(to_lon, to_lat):
        pl.semaphore_signal(barrier, inc=1, device_id=(to_lon, to_lat), device_id_type=MESH)

    greet(sides[0], lat)
    greet(sides[2], lat)
    for s in range(2):
        @pl.when(has[s])
        def _():
            for t in range(3):
                greet(sides[t], lat + 2 * s - 1)

    f_at, c_at, i_at = 0, kf * lons, kf * lons + kc * halves
    loads[0].wait()
    wide[c_at:c_at + kc * halves] = coarse_in[...].astype(F32)
    coarse_own = []
    for c in range(halves):
        values = wide[pl.ds(c_at + c, kc, stride=halves), :]
        own_c[c * kc:(c + 1) * kc] = values.astype(BF16)
        coarse_own.append(values)

    for s in range(2):
        @pl.when(jnp.logical_not(has[s]))
        def _():
            rim_in[s] = jnp.zeros(rim_in.shape[1:], BF16)

    one = jnp.int32(1)
    pl.semaphore_wait(
        barrier, 2 + 3 * jnp.where(has[0], one, 0) + 3 * jnp.where(has[1], one, 0)
    )

    def send(src, dst, n, towards):
        return pltpu.make_async_remote_copy(
            src_ref=src, dst_ref=dst, send_sem=send_sem.at[n], recv_sem=recv_sem.at[n],
            device_id=(sides[towards], lat), device_id_type=MESH,
        )

    coarse_west = send(own_c, east_cin, 0, 0)
    coarse_east = send(own_c, west_cin, 1, 2)
    rest_west = send(own.at[pl.ds(0, body)], east, 2, 0)
    rest_east = send(own.at[pl.ds(col, body)], west, 3, 2)
    coarse_east.start()
    coarse_west.start()

    fine_own, inc_own = [], []
    loads[1].wait()
    wide[f_at:f_at + kf * lons] = fine_in[...].astype(F32)
    for a in range(lons):
        values = wide[pl.ds(f_at + a, kf, stride=lons), :]
        anom = (values - jnp.mean(values, axis=0, keepdims=True)).astype(BF16)
        own[a * col:a * col + kf] = anom
        fine_own.append(anom)
    loads[2].wait()
    wide[i_at:i_at + nv * lons] = inc_in[...].astype(F32)
    for a in range(lons):
        vectors = wide[pl.ds(i_at + a, nv, stride=lons), :].astype(BF16)
        own[a * col + kf:(a + 1) * col] = vectors
        inc_own.append(vectors)

    rest_east.start()
    rest_west.start()
    lane = iota((kf, lats), 1)
    packs = (
        [v.astype(F32) for v in fine_own] + [v.astype(F32) for v in inc_own],
        [coarse_own[c][g * kf:(g + 1) * kf] for g in range(groups) for c in range(halves)],
    )
    for part in range(2):
        low = high = jnp.zeros((kf, lats), F32)
        for q, values in enumerate(packs[part]):
            here = (lane // reach) == q
            low = jnp.where(here, pltpu.roll(values, (reach * q) % lats, 1), low)
            high = jnp.where(here, pltpu.roll(values, (reach * (q + 1)) % lats, 1), high)
        rim_out[0, part * kf:(part + 1) * kf] = low.astype(BF16)
        rim_out[1, part * kf:(part + 1) * kf] = high.astype(BF16)

    def rim_copy(s, t):
        return pltpu.make_async_remote_copy(
            src_ref=rim_out.at[s], dst_ref=rim_in.at[1 - s, 2 - t],
            send_sem=rim_send_sem.at[s, t], recv_sem=rim_recv_sem.at[1 - s, 2 - t],
            device_id=(sides[t], lat + 2 * s - 1), device_id_type=MESH,
        )

    for s in range(2):
        @pl.when(has[s])
        def _():
            for t in (2, 0, 1):
                rim_copy(s, t).start()


    loads[3].wait()
    w_coarse = w_ref[1] / (kc - 1)
    fine_ratio = ratio * w_ref[0] / w_ref[1]
    lat_profile = w_coarse * profile(iota((lats, lats), 0) - iota((lats, lats), 1), reach)
    for d in range(lon_reach + 1):
        taper[d] = lat_profile * (1.0 - 0.75 * (d / lon_reach) * (d / lon_reach))

    block = lons * reach
    shape = (2 * block, lats)
    row, lane = iota(shape, 0), iota(shape, 1)
    side, a_row, i_row = row // block, (row % block) // reach, row % reach
    b_lane, l_lane = lane // reach, lane % reach
    for s in range(2):
        d_lat = i_row - l_lane + reach if s == 0 else reach + l_lane - i_row
        in_lat = jnp.where((side == s) & (b_lane < lons), w_coarse * profile(d_lat, reach), 0.0)
        for t in range(3):
            d_lon = (t - 1) * lons + b_lane - a_row
            n = 2 * t + s
            rim_taper[:, n * lats:(n + 1) * lats] = in_lat * profile(d_lon, lon_reach)

    shape = (2 * lats, lats)
    row, lane = iota(shape, 0), iota(shape, 1)
    place = (row // lats) * halves + (row // reach) % halves
    step = jnp.abs(2 * place - lane // reach)
    weight = jnp.where(step == 0, 1.0, jnp.where(step == 1, 0.5, 0.0))
    weight = jnp.where((row % reach == lane % reach) & (lane < block), weight, 0.0)
    for g in range(groups):
        mine = (row % lats) // (reach * halves) == g
        refine_rim[:, g * lats:(g + 1) * lats] = jnp.where(mine, weight, 0.0).astype(BF16)

    def coarse_parts(refined):
        coarse_anom = refined - jnp.mean(refined, axis=0, keepdims=True)
        pair = refined[:kf]
        paired = pair - jnp.mean(pair, axis=0, keepdims=True)
        return coarse_anom.astype(BF16), paired.astype(BF16)

    def lanes_of(b):
        return slice((b + lon_reach) * lats, (b + lon_reach + 1) * lats)

    def set_near(to, lanes, refined):
        coarse_anom, paired = coarse_parts(refined)
        to[2 * kf:2 * kf + kc, lanes] = coarse_anom
        to[2 * kf + kc:3 * kf + kc, lanes] = paired
        to[3 * kf + kc:, lanes] = paired
        return coarse_anom, paired

    def set_fine(b, fine_anom, vectors):
        near[:kf, lanes_of(b)] = fine_anom
        near[kf:2 * kf, lanes_of(b)] = fine_anom
        near_inc[:, lanes_of(b)] = vectors

    def split(scale, values):
        scaled = scale * values.astype(F32)
        high = scaled.astype(BF16).astype(F32)
        return [high, scaled - high]

    def set_own(a, refined):
        coarse_anom, paired = set_near(near, lanes_of(a), refined)
        set_fine(a, fine_own[a], inc_own[a])
        parts = split(fine_ratio, fine_own[a]) + [coarse_anom.astype(F32)] + split(-ratio, paired)
        own_t[a * lats:(a + 1) * lats] = jnp.concatenate(parts, axis=0).T.astype(BF16)

    def add(b, first, last):
        lanes = lanes_of(b)
        gram = jnp.dot(
            own_t[first * lats:last * lats], near[:, lanes], preferred_element_type=F32
        )
        tapered = jnp.concatenate(
            [
                (gram[(a - first) * lats:(a - first + 1) * lats] * taper[abs(a - b)]).astype(BF16)
                for a in range(first, last)
            ],
            axis=0,
        )
        acc[:, first * lats:last * lats] += lax.dot_general(
            near_inc[:, lanes], tapered, (((1,), (1,)), ((), ())), preferred_element_type=F32
        )

    acc[...] = jnp.zeros_like(acc)
    for a in range(lon_reach):
        left = coarse_own[a // 2]
        set_own(a, left if a % 2 == 0 else 0.5 * (left + coarse_own[a // 2 + 1]))
    for b in range(lon_reach):
        add(b, 0, lon_reach)

    def rim_pack(s, t):
        return jnp.concatenate((rim_in[s, t, kf:], rim_in[s, min(t + 1, 2), kf:]), axis=1)

    def wait_rims(some):
        for s in range(2):
            @pl.when(has[s])
            def _():
                for t in some:
                    rim_copy(1 - s, 2 - t).wait_recv()

    def set_rims(some):
        order = [(s, t) for s in range(2) for t in some]
        refined_rim = jnp.dot(
            jnp.concatenate([rim_pack(s, t) for s, t in order], axis=0),
            refine_rim[...],
            preferred_element_type=F32,
        )
        for n, (s, t) in enumerate(order):
            lanes = slice((2 * t + s) * lats, (2 * t + s + 1) * lats)
            refined = jnp.concatenate(
                [
                    refined_rim[n * kf:(n + 1) * kf, g * lats:(g + 1) * lats]
                    for g in range(groups)
                ],
                axis=0,
            )
            set_near(near_rim, lanes, refined)
            near_rim[:kf, lanes] = rim_in[s, t, :kf]
            near_rim[kf:2 * kf, lanes] = rim_in[s, t, :kf]
            rim_inc[:, lanes] = pltpu.roll(
                rim_in[s, t, :kf].astype(F32), lats - block, 1
            ).astype(BF16)

    def rim_product(first, last):
        lanes = slice(2 * first * lats, 2 * last * lats)
        gram = jnp.dot(own_rim, near_rim[:, lanes], preferred_element_type=F32)
        tapered = (gram * rim_taper[:, lanes]).astype(BF16)
        return lax.dot_general(
            rim_inc[:, lanes], tapered, (((1,), (1,)), ((), ())), preferred_element_type=F32
        )

    coarse_west.wait_recv()
    east_c = [east_cin[c * kc:(c + 1) * kc].astype(F32) for c in range(halves)]
    set_own(lon_reach, 0.5 * (coarse_own[halves - 1] + east_c[0]))
    add(lon_reach, 0, lons)
    for b in range(lon_reach):
        add(b, lon_reach, lons)
    for b in range(lon_reach):
        left = east_c[b // 2]
        refined = left if b % 2 == 0 else 0.5 * (left + east_c[b // 2 + 1])
        set_near(near, lanes_of(lons + b), refined)
    own_rim = jnp.concatenate(
        [
            own_t[a * lats + s * (lats - reach):a * lats + s * (lats - reach) + reach]
            for s in range(2)
            for a in range(lons)
        ],
        axis=0,
    )

    coarse_east.wait_recv()
    west_c = [west_cin[c * kc:(c + 1) * kc].astype(F32) for c in range(halves)]
    west_c.append(coarse_own[0])
    for b in range(1, lons):
        left = west_c[b // 2]
        refined = left if b % 2 == 0 else 0.5 * (left + west_c[b // 2 + 1])
        set_near(near, lanes_of(b - lons), refined)

    rest_west.wait_recv()
    wait_rims((1, 2))
    for b in range(lon_reach):
        at = b * col
        set_fine(lons + b, east[at:at + kf], east[at + kf:at + col])
        add(lons + b, b + 1, lons)
    set_rims((1, 2))
    edge = rim_product(1, 3)

    rest_east.wait_recv()
    wait_rims((0,))
    for b in range(1, lons):
        at = (b - 1) * col
        set_fine(b - lons, west[at:at + kf], west[at + kf:at + col])
        add(b - lons, 0, b)
    set_rims((0,))
    edge += rim_product(0, 1)

    lane = iota((nv, lats), 1)
    for a in range(lons):
        low = pltpu.roll(edge, (lats - reach * a) % lats, 1)
        high = pltpu.roll(edge, (2 * lats - reach - block - reach * a) % lats, 1)
        total = acc[:, a * lats:(a + 1) * lats]
        total += jnp.where(lane < reach, low, 0.0) + jnp.where(lane >= lats - reach, high, 0.0)
        out_ref[pl.ds(a, nv, stride=lons), :] = total

    for copy in (coarse_west, coarse_east, rest_west, rest_east):
        copy.wait_send()
    for s in range(2):
        @pl.when(has[s])
        def _():
            for t in range(3):
                rim_copy(s, t).wait_send()


def solution(mesh):
    n_lon, n_lat = mesh.shape["lon"], mesh.shape["lat"]

    def per_device(fine, coarse, inc, weights):
        kf, lons, lats = fine.shape
        kc, halves, _ = coarse.shape
        nv = inc.shape[0]
        members, col, near_lons = 4 * kf + kc, kf + nv, 3 * lons - 2
        body = (lons - 1) * col
        assert nv == kf and 2 * lons * (lats // 8) == lats and kc * halves == 2 * lons * kf
        result = pl.pallas_call(
            functools.partial(kernel, (n_lon, n_lat, kf, kc, nv, lons, lats)),
            out_shape=pltpu.VMEM((nv * lons, lats), F32),
            in_specs=[pl.BlockSpec(memory_space=pl.ANY)] * 4,
            out_specs=pl.BlockSpec(memory_space=pltpu.VMEM),
            scratch_shapes=[
                pltpu.SMEM(weights.shape, F32),
                pltpu.VMEM((kf * lons, lats), BF16),
                pltpu.VMEM((kc * halves, lats), BF16),
                pltpu.VMEM((nv * lons, lats), BF16),
                pltpu.VMEM((col * lons + kc * halves, lats), F32),
                pltpu.VMEM((body + col, lats), BF16),
                pltpu.VMEM((kc * halves, lats), BF16),
                pltpu.VMEM((body, lats), BF16),
                pltpu.VMEM((body, lats), BF16),
                pltpu.VMEM((kc * halves, lats), BF16),
                pltpu.VMEM((kc * halves, lats), BF16),
                pltpu.VMEM((2, 2 * kf, lats), BF16),
                pltpu.VMEM((2, 3, 2 * kf, lats), BF16),
                pltpu.VMEM((members, near_lons * lats), BF16),
                pltpu.VMEM((nv, near_lons * lats), BF16),
                pltpu.VMEM((lons * lats, members), BF16),
                pltpu.VMEM((members, 6 * lats), BF16),
                pltpu.VMEM((nv, 6 * lats), BF16),
                pltpu.VMEM((lons, lats, lats), F32),
                pltpu.VMEM((lats, 6 * lats), F32),
                pltpu.VMEM((2 * lats, (kc // kf) * lats), BF16),
                pltpu.VMEM((nv, lons * lats), F32),
                pltpu.SemaphoreType.DMA((4,)),
                pltpu.SemaphoreType.DMA((4,)),
                pltpu.SemaphoreType.DMA((4,)),
                pltpu.SemaphoreType.DMA((2, 3)),
                pltpu.SemaphoreType.DMA((2, 3)),
            ],
            compiler_params=pltpu.CompilerParams(collective_id=0, has_side_effects=True),
            name="covariance",
        )(
            weights,
            fine.reshape(kf * lons, lats),
            coarse.reshape(kc * halves, lats),
            inc.reshape(nv * lons, lats),
        )
        return result.reshape(nv, lons, lats)

    spec = P(None, "lon", "lat")
    return jax.shard_map(
        per_device, mesh=mesh, in_specs=(spec, spec, spec, P()), out_specs=spec, check_vma=False
    )
```
